256 devices in a mesh: row: 16 (over x, z_lo), col: 16 (over y, z_hi, core).
Axes of the slice: x: 4, y: 4, z: 8 (z_hi: 2, z_lo: 4; z = z_hi * 4 + z_lo), core: 2. Of those that a mesh axis runs over, the one named last changes fastest.
Arguments:
- t2_amps: bfloat16 [16384, 49152], P('row', 'col'), may hold values from -0.5 to 0.5
- l2_amps: bfloat16 [512, 49152], P('row', 'col'), may hold values from -0.02734375 to 0.02734375
Outputs:
- ladder: bfloat16 [512, 49152], P('row', 'col')
The draws below stay inside these ranges and needn't reach their ends.
All inputs are finite; a program needn't handle non-finite values.
Results may differ from the reference program's by a relative error of at most 0.0044.
Values may be sent and summed in bfloat16 or wider, within the bound.
No kernel may reach another device: no remote copies, remote signals or barrier semaphores. Data moves between devices by JAX's collectives and lax.ppermute only.
A program may use at most 64 MiB of HBM per device.

```python
import jax
import jax.numpy as jnp

O = 128
OO = 16384
PV = 49152
KL = 512


def block_levels(own_key, shape, shards, low, largest):
    def one(position, parts):
        draws = jax.random.uniform(jax.random.fold_in(jax.random.fold_in(own_key, 6), position), (parts,), jnp.float32, low / len(shards), largest / len(shards))
        return jnp.repeat(jnp.exp(draws), shape[position] // parts).reshape((-1,) + (1,) * (len(shape) - position - 1))

    factor_of = one(*shards[0])
    for cut in shards[1:]:
        factor_of = factor_of * one(*cut)
    return factor_of


def gaussian(key, extent, width, most, cuts=(), kind=jnp.bfloat16):
    values = jax.random.normal(key, extent, jnp.float32) * width
    if len(cuts) > 0:
        values = block_levels(key, extent, cuts, -0.22, 0.18) * values
    return jnp.clip(values, min=-most, max=most).astype(kind)


def setup_inputs(seed: int = 0) -> dict:
    splits = jax.random.split(jax.random.key(seed), 3)
    return {
        "t2_amps": gaussian(splits[0], (OO, PV), O ** -0.5, 0.5, ((0, 16), (1, 16))),
        "l2_amps": gaussian(splits[1], (KL, PV), PV ** -0.5, 0.02734375, ((0, 16), (1, 16))),
    }


def reference(t2_amps, l2_amps):
    oooo = jnp.dot(t2_amps, l2_amps.T, preferred_element_type=jnp.float32)
    oooo_half = oooo.astype(jnp.bfloat16)
    ladder = jnp.dot(oooo_half.T, t2_amps, preferred_element_type=jnp.float32)
    return ladder.astype(jnp.bfloat16)
```

```python
import jax
import jax.numpy as jnp
from jax import lax
from jax.experimental import pallas as pl
from jax.experimental.pallas import tpu as pltpu
from jax.sharding import Mesh
from jax.sharding import PartitionSpec as P


ROW = ("x", "zl")
COL = ("y", "zh", "c")
SIZE = {"x": 4, "zl": 4, "y": 4, "zh": 2, "c": 2}
BF16 = jnp.bfloat16
F32 = jnp.float32
ROWS = 32
CHUNKS = ((((0,), (1,)), ((1, 0),)), (((3,), (2,)), ((2,), (3,))))
RELAY_A = set()
RELAY_C = {(1, 0)}


def shift(value, axis, by):
    size = SIZE[axis]
    return lax.ppermute(value, axis, [(i, (i + by) % size) for i in range(size)])


def halves(value):
    rows = value.shape[0] // 2
    return value[:rows], value[rows:]


def gather_x(block, group):
    left = shift(block, "x", 1)
    right = shift(block, "x", -1)
    if group in RELAY_A:
        far = jnp.concatenate([shift(halves(left)[0], "x", 1), shift(halves(right)[1], "x", -1)])
    else:
        far = shift(block, "x", 2)
    return jnp.concatenate([block, left, right, far])


def sum_x(part, sends, at, group):
    def rows(value, dx):
        return jnp.concatenate([value[at(dx, k) : at(dx, k) + ROWS] for k in group])

    if group in RELAY_C:
        low, high = halves(rows(sends, 3))
        to_right = shift(low, "x", 1)
        to_left = shift(high, "x", -1)
        low = (halves(rows(part, 2))[0] + to_right.astype(F32)).astype(BF16)
        high = (halves(rows(part, 1))[1] + to_left.astype(F32)).astype(BF16)
        right16 = jnp.concatenate([low, halves(rows(sends, 2))[1]])
        left16 = jnp.concatenate([halves(rows(sends, 1))[0], high])
        total = rows(part, 0)
    else:
        right16, left16 = rows(sends, 2), rows(sends, 1)
        total = rows(part, 0) + shift(rows(sends, 3), "x", 2).astype(F32)
    total = total + shift(right16, "x", 1).astype(F32)
    return total + shift(left16, "x", -1).astype(F32)


def turn(t2_ref, out_ref, sems):
    y = lax.axis_index("y")
    c = lax.axis_index("c")
    rows = out_ref.shape[0] // 8
    copies = []
    for half in range(2):
        for r in range(4):
            source = lax.rem(c + half, 2) * 4 + lax.rem(y + 4 - r, 4)
            slot = half * 4 + r
            copies.append(
                pltpu.make_async_copy(
                    t2_ref.at[pl.ds(pl.multiple_of(source * rows, rows), rows)],
                    out_ref.at[pl.ds(slot * rows, rows)],
                    sems.at[slot],
                )
            )
    for copy in copies:
        copy.start()
    for copy in copies:
        copy.wait()


def turned(t2):
    return pl.pallas_call(
        turn,
        out_shape=pltpu.VMEM(t2.shape, t2.dtype),
        in_specs=[pl.BlockSpec(memory_space=pltpu.HBM)],
        out_specs=pl.BlockSpec(memory_space=pltpu.VMEM),
        compiler_params=pltpu.CompilerParams(vmem_limit_bytes=1 << 20),
        scratch_shapes=[pltpu.SemaphoreType.DMA((8,))],
        cost_estimate=pl.CostEstimate(flops=1000000, bytes_accessed=2 * t2.size * 2, transcendentals=0),
        name="turn",
    )(t2)


def all_sum(partial):
    mine, theirs = halves(partial)
    other = shift(theirs, "c", 1)
    mine = mine + other
    sends = mine.astype(BF16)
    rows = mine.shape[0] // 4
    quarter = [sends[r * rows : (r + 1) * rows] for r in range(4)]
    got = [shift(quarter[4 - k], "y", k) for k in (1, 3, 2)]
    total = mine[:rows] + got[0].astype(F32) + got[1].astype(F32) + got[2].astype(F32)
    total16 = total.astype(BF16)
    other = shift(total16, "zh", 1)
    own = (total + other.astype(F32)).astype(BF16)
    others = {k: shift(own, "y", k) for k in (1, 3, 2)}
    half = jnp.concatenate([own, others[1], others[2], others[3]])
    return jnp.concatenate([half, shift(half, "c", 1)])


def on_device(t2, l2):
    t2 = turned(t2)
    by_z = {0: l2} | {k: shift(l2, "zl", k) for k in (1, 3, 2)}
    sums = {}
    for a_groups, c_groups in CHUNKS:
        blocks = [gather_x(jnp.concatenate([by_z[k] for k in g]), g) for g in a_groups]
        partial = lax.dot_general(
            t2, jnp.concatenate(blocks), (((1,), (1,)), ((), ())), preferred_element_type=F32
        )
        half = all_sum(partial)
        part = lax.dot_general(
            half, t2, (((0,), (0,)), ((), ())), preferred_element_type=F32
        )
        sends = part.astype(BF16)

        def at(dx, k):
            start = 0
            for g in a_groups:
                if k in g:
                    return start + ROWS * (dx * len(g) + g.index(k))
                start += 4 * ROWS * len(g)

        for group in c_groups:
            done = sum_x(part, sends, at, group)
            if group != c_groups[-1]:
                part, done = lax.optimization_barrier((part, done))
            for i, k in enumerate(group):
                sums[k] = done[i * ROWS : (i + 1) * ROWS]
    total = sums[0]
    for k in (1, 2, 3):
        total = total + shift(sums[k].astype(BF16), "zl", -k).astype(F32)
    return total.astype(BF16)


def solution(mesh):
    finer = Mesh(mesh.devices.reshape(4, 4, 4, 2, 2), ROW + COL)
    return jax.shard_map(
        on_device,
        mesh=finer,
        in_specs=(P(ROW, COL), P(ROW, COL)),
        out_specs=P(ROW, COL),
        check_vma=False,
    )
```

```python
import jax
import jax.numpy as jnp
from jax import lax
from jax.experimental import pallas as pl
from jax.experimental.pallas import tpu as pltpu
from jax.sharding import Mesh
from jax.sharding import PartitionSpec as P


ROW = ("x", "zl")
COL = ("y", "zh", "c")
SIZE = {"x": 4, "zl": 4, "y": 4, "zh": 2, "c": 2}
BF16 = jnp.bfloat16
F32 = jnp.float32
ROWS = 32
CHUNKS = ((((0,), (1,)), ((1, 0),)), (((3,), (2,)), ((2,), (3,))))
RELAY_A = set()
RELAY_C = {(1, 0)}


def shift(value, axis, by):
    size = SIZE[axis]
    return lax.ppermute(value, axis, [(i, (i + by) % size) for i in range(size)])


def swap(value, axis, by):
    return lax.ppermute(value, axis, [(i, i ^ by) for i in range(4)])


def halves(value):
    rows = value.shape[0] // 2
    return value[:rows], value[rows:]


def gather_x(block, group):
    left = swap(block, "x", 1)
    right = swap(block, "x", 3)
    if group in RELAY_A:
        far = jnp.concatenate([swap(halves(left)[0], "x", 3), swap(halves(right)[1], "x", 1)])
    else:
        far = swap(block, "x", 2)
    return jnp.concatenate([block, left, right, far])


def sum_x(part, sends, at, group):
    def rows(value, dx):
        return jnp.concatenate([value[at(dx, k) : at(dx, k) + ROWS] for k in group])

    if group in RELAY_C:
        low, high = halves(rows(sends, 3))
        to_right = swap(low, "x", 1)
        to_left = swap(high, "x", 3)
        low = (halves(rows(part, 2))[0] + to_right.astype(F32)).astype(BF16)
        high = (halves(rows(part, 1))[1] + to_left.astype(F32)).astype(BF16)
        right16 = jnp.concatenate([low, halves(rows(sends, 2))[1]])
        left16 = jnp.concatenate([halves(rows(sends, 1))[0], high])
        total = rows(part, 0)
    else:
        right16, left16 = rows(sends, 2), rows(sends, 1)
        total = rows(part, 0) + swap(rows(sends, 3), "x", 2).astype(F32)
    total = total + swap(right16, "x", 3).astype(F32)
    return total + swap(left16, "x", 1).astype(F32)


def turn(t2_ref, out_ref, sems):
    y = lax.axis_index("y")
    c = lax.axis_index("c")
    rows = out_ref.shape[0] // 8
    copies = []
    for half in range(2):
        for r in range(4):
            high = lax.rem(lax.div(y, 2) + r // 2, 2)
            low = lax.rem(y + r % 2, 2)
            source = lax.rem(c + half, 2) * 4 + high * 2 + low
            slot = half * 4 + r
            copies.append(
                pltpu.make_async_copy(
                    t2_ref.at[pl.ds(pl.multiple_of(source * rows, rows), rows)],
                    out_ref.at[pl.ds(slot * rows, rows)],
                    sems.at[slot],
                )
            )
    for copy in copies:
        copy.start()
    for copy in copies:
        copy.wait()


def turned(t2):
    return pl.pallas_call(
        turn,
        out_shape=pltpu.VMEM(t2.shape, t2.dtype),
        in_specs=[pl.BlockSpec(memory_space=pltpu.HBM)],
        out_specs=pl.BlockSpec(memory_space=pltpu.VMEM),
        compiler_params=pltpu.CompilerParams(vmem_limit_bytes=1 << 20),
        scratch_shapes=[pltpu.SemaphoreType.DMA((8,))],
        cost_estimate=pl.CostEstimate(flops=1000000, bytes_accessed=2 * t2.size * 2, transcendentals=0),
        name="turn",
    )(t2)


def all_sum(partial):
    mine, theirs = halves(partial)
    other = shift(theirs, "c", 1)
    mine = mine + other
    sends = mine.astype(BF16)
    rows = mine.shape[0] // 4
    quarter = [sends[r * rows : (r + 1) * rows] for r in range(4)]
    got = [swap(quarter[k], "y", k) for k in (1, 3, 2)]
    total = mine[:rows] + got[0].astype(F32) + got[1].astype(F32) + got[2].astype(F32)
    total16 = total.astype(BF16)
    other = shift(total16, "zh", 1)
    own = (total + other.astype(F32)).astype(BF16)
    others = {k: swap(own, "y", k) for k in (1, 3, 2)}
    half = jnp.concatenate([own, others[1], others[2], others[3]])
    return jnp.concatenate([half, shift(half, "c", 1)])


def on_device(t2, l2):
    t2 = turned(t2)
    by_z = {0: l2} | {k: shift(l2, "zl", k) for k in (1, 3, 2)}
    sums = {}
    for a_groups, c_groups in CHUNKS:
        blocks = [gather_x(jnp.concatenate([by_z[k] for k in g]), g) for g in a_groups]
        partial = lax.dot_general(
            t2, jnp.concatenate(blocks), (((1,), (1,)), ((), ())), preferred_element_type=F32
        )
        half = all_sum(partial)
        part = lax.dot_general(
            half, t2, (((0,), (0,)), ((), ())), preferred_element_type=F32
        )
        sends = part.astype(BF16)

        def at(dx, k):
            start = 0
            for g in a_groups:
                if k in g:
                    return start + ROWS * (dx * len(g) + g.index(k))
                start += 4 * ROWS * len(g)

        for group in c_groups:
            done = sum_x(part, sends, at, group)
            if group != c_groups[-1]:
                part, done = lax.optimization_barrier((part, done))
            for i, k in enumerate(group):
                sums[k] = done[i * ROWS : (i + 1) * ROWS]
    total = sums[0]
    for k in (1, 2, 3):
        total = total + shift(sums[k].astype(BF16), "zl", -k).astype(F32)
    return total.astype(BF16)


def solution(mesh):
    finer = Mesh(mesh.devices.reshape(4, 4, 4, 2, 2), ROW + COL)
    return jax.shard_map(
        on_device,
        mesh=finer,
        in_specs=(P(ROW, COL), P(ROW, COL)),
        out_specs=P(ROW, COL),
        check_vma=False,
    )
```
